32 devices in a mesh: rows: 2 (over x), cols: 4 (over z), slabs: 2 (over y), trial: 2 (over core).
Axes of the slice: x: 2, y: 2, z: 4, core: 2. Of those that a mesh axis runs over, the one named last changes fastest.
Arguments:
- field_values: float32 [32, 64, 128, 128], P(('trial', 'rows'), 'cols', 'slabs'), parts along dimension 0, may hold values from 0.2 to 1.8
- crowding: float32 [32, 64, 128, 128], P(('trial', 'rows'), 'cols', 'slabs'), parts along dimension 0, may hold values from 0.5 to 2
Outputs:
- potential: float32 [32, 64, 128, 128], P(('trial', 'rows'), 'cols', 'slabs'), parts along dimension 0
- field_values_end: float32 [32, 64, 128, 128], P(('trial', 'rows'), 'cols', 'slabs'), parts along dimension 0
The draws below stay inside these ranges and needn't reach their ends.
There are 2 independent parts, one for each index of `trial`. The reference program is written for one: setup_inputs(seed, part) draws one part's arguments, and reference() takes and returns one part's arrays. A program takes and returns all parts, laid end to end along the dimension named above; each array names one. Nothing has to cross between parts.
All inputs are finite; a program needn't handle non-finite values.
Results may differ from the reference program's by a relative error of at most 0.00002.
Values sent between devices are 32-bit elements; how exact they have to be, the bound alone decides.
A program may use at most 64 MiB of HBM per device.

```python
import jax
import jax.numpy as jnp
from jax import lax

GRID_J = 16
GRID_I = 64
GRID_K = 128
LEVELS = 128
STEPS = 3


def block_levels(rng, shape, pieces, least, top_value):
    factor_of = 1.0
    for axis_at, parts in pieces:
        steps = jax.random.uniform(jax.random.fold_in(jax.random.fold_in(rng, 6), axis_at), (parts,), jnp.float32, least / len(pieces), top_value / len(pieces))
        factor_of = factor_of * jnp.repeat(jnp.exp(steps), shape[axis_at] // parts).reshape((-1,) + (1,) * (len(shape) - 1 - axis_at))
    return factor_of


def setup_inputs(seed: int = 0, part: int = 0) -> dict:
    keys = jax.random.split(jax.random.key(seed), 3)
    part_splits = jax.random.split(jax.random.fold_in(keys[2], part), 3)
    return {
        "field_values": jnp.clip(0.2 + 1.5999999 * jax.random.uniform(part_splits[0], (GRID_J, GRID_I, GRID_K, LEVELS), jnp.float32) ** block_levels(part_splits[0], (GRID_J, GRID_I, GRID_K, LEVELS), ((0, 2), (1, 4), (2, 2)), -0.2, 0.2), 0.2, 1.8),
        "crowding": jnp.clip(0.5 + 1.5 * jax.random.uniform(part_splits[1], (GRID_J, GRID_I, GRID_K, LEVELS), jnp.float32) ** block_levels(part_splits[1], (GRID_J, GRID_I, GRID_K, LEVELS), ((0, 2), (1, 4), (2, 2)), -0.2, 0.2), 0.5, 2.0),
    }


def without_rim(values, dims):
    for dim in dims:
        values = lax.slice_in_dim(values, 1, values.shape[dim] - 1, axis=dim)
    return values


def shifted_cells(values, dim, start, dims):
    others = [other for other in dims if other != dim]
    values = without_rim(values, others)
    return lax.slice_in_dim(values, start, start + values.shape[dim] - 2, axis=dim)


def march_step(padded, crowding):
    middle = without_rim(padded, (0, 1, 2))
    lower = [shifted_cells(padded, dim, 0, (0, 1, 2)) for dim in (0, 1, 2)]
    upper = [shifted_cells(padded, dim, 2, (0, 1, 2)) for dim in (0, 1, 2)]
    spread = lower[0] + upper[0] + lower[1] + upper[1] + lower[2] + upper[2] - 6.0 * middle
    return middle + 0.1 * spread + 0.2 * middle * (1.0 - middle * crowding)


def reference(field_values, crowding):
    for step in range(STEPS):
        field_values = march_step(jnp.pad(field_values, ((1, 1), (1, 1), (1, 1), (0, 0)), mode="constant"), crowding)
    potential = jnp.cumsum(field_values, axis=0) / GRID_J
    return potential, field_values
```

```python
import functools

import jax
import jax.numpy as jnp
from jax import lax
from jax.experimental import pallas as pl
from jax.experimental.pallas import tpu as pltpu
from jax.sharding import PartitionSpec as P

STEPS = 3
MESH = pl.DeviceIdType.MESH
AXES = ("rows", "cols", "slabs")


def pieces_of(length):
    for count in (4, 2):
        if length % count == 0:
            return count
    return 1


def march_kernel(
    sizes, field, crowd, out_field, out_below,
    grid0, grid1, grid2, grid3, cells, y_in, y_out, total, below,
    x_send, x_recv, z_send, z_recv, y_send, y_recv, t_send, t_recv, load, store,
):
    J, I, K, L = field.shape
    grids = (grid0, grid1, grid2, grid3)
    Q = pieces_of(I)
    W = I // Q
    place = {axis: lax.axis_index(axis) for axis in AXES}
    has_target = {}
    has_source = {}
    for axis in AXES:
        later, earlier = place[axis] < sizes[axis] - 1, place[axis] > 0
        has_target[axis] = (later, earlier)
        has_source[axis] = (earlier, later)

    def target(axis, way):
        n = sizes[axis]
        return {axis: lax.rem(place[axis] + (1 if way == 0 else n - 1), n)}

    load_field = pltpu.make_async_copy(
        field, grid0.at[1 : J + 1, 1 : I + 1], load.at[0]
    )
    load_cells = pltpu.make_async_copy(crowd, cells, load.at[1])
    load_field.start()

    barrier = pltpu.get_barrier_semaphore()
    for axis in AXES:
        if sizes[axis] > 1:
            for way in (0, 1):

                @pl.when(has_target[axis][way])
                def _():
                    pl.semaphore_signal(
                        barrier, inc=1, device_id=target(axis, way), device_id_type=MESH
                    )

    peers = jnp.int32(0)
    for axis in AXES:
        if sizes[axis] > 1:
            for way in (0, 1):
                peers = peers + has_source[axis][way].astype(jnp.int32)
    pl.semaphore_wait(barrier, peers)

    def x_copy(step, way, q):
        plane = J - 1 if way == 0 else 0
        halo = 0 if way == 0 else J + 1
        columns = pl.ds(1 + q * W, W)
        if step == 0:
            source = field.at[plane, pl.ds(q * W, W)]
        else:
            source = grids[step].at[1 + plane, columns]
        return pltpu.make_async_remote_copy(
            src_ref=source,
            dst_ref=grids[step].at[halo, columns],
            send_sem=x_send.at[step, way, q],
            recv_sem=x_recv.at[step, way, q],
            device_id=target("rows", way),
            device_id_type=MESH,
        )

    parts = ((0, 1), (1, J - 2), (J - 1, 1))

    def z_copy(step, way, part):
        first, count = parts[part]
        column = I - 1 if way == 0 else 0
        halo = 0 if way == 0 else I + 1
        if step == 0:
            source = field.at[pl.ds(first, count), column]
        else:
            source = grids[step].at[pl.ds(1 + first, count), 1 + column]
        return pltpu.make_async_remote_copy(
            src_ref=source,
            dst_ref=grids[step].at[pl.ds(1 + first, count), halo],
            send_sem=z_send.at[step, way, part],
            recv_sem=z_recv.at[step, way, part],
            device_id=target("cols", way),
            device_id_type=MESH,
        )

    def y_copy(step, way):
        return pltpu.make_async_remote_copy(
            src_ref=y_out.at[step, 1 - way],
            dst_ref=y_in.at[step, way],
            send_sem=y_send.at[step, way],
            recv_sem=y_recv.at[step, way],
            device_id=target("slabs", way),
            device_id_type=MESH,
        )

    def t_copy(q):
        columns = pl.ds(q * W, W)
        return pltpu.make_async_remote_copy(
            src_ref=total.at[columns],
            dst_ref=below.at[columns],
            send_sem=t_send.at[q],
            recv_sem=t_recv.at[q],
            device_id=target("rows", 0),
            device_id_type=MESH,
        )

    def start(axis, way, copies):
        if sizes[axis] > 1:

            @pl.when(has_target[axis][way])
            def _():
                for one in copies:
                    one.start()

    def sent(axis, way, copies):
        if sizes[axis] > 1:

            @pl.when(has_target[axis][way])
            def _():
                for one in copies:
                    one.wait_send()

    def arrived(axis, way, copies):
        if sizes[axis] > 1:

            @pl.when(has_source[axis][way])
            def _():
                for one in copies:
                    one.wait_recv()

    for way in (0, 1):
        start("cols", way, [z_copy(0, way, part) for part in range(3)])
    for q in range(Q):
        for way in (0, 1):
            start("rows", way, [x_copy(0, way, q)])
    load_cells.start()

    zero = jnp.zeros((K, L), jnp.float32)
    for way in (0, 1):

        @pl.when(jnp.logical_not(has_source["rows"][way]))
        def _():
            def body(i, _):
                for step in range(STEPS):
                    grids[step][0 if way == 0 else J + 1, 1 + i] = zero
                if way == 0:
                    below[i] = zero
                return 0

            lax.fori_loop(0, I, body, 0)

        @pl.when(jnp.logical_not(has_source["cols"][way]))
        def _():
            def body(j, _):
                for step in range(STEPS):
                    grids[step][1 + j, 0 if way == 0 else I + 1] = zero
                return 0

            lax.fori_loop(0, J, body, 0)

        @pl.when(jnp.logical_not(has_source["slabs"][way]))
        def _():
            for step in range(STEPS):
                y_in[step, way] = jnp.zeros((J, I, L), jnp.float32)

    load_field.wait()

    def rims(step, j, i, value):
        y_out[step, 0, j, pl.ds(i, 1), :] = value[0:1]
        y_out[step, 1, j, pl.ds(i, 1), :] = value[K - 1 : K]

    def first_rims(j, _):
        def body(i, _):
            for side, row in ((0, 0), (1, K - 1)):
                y_out[0, side, j, pl.ds(i, 1), :] = grid0[1 + j, 1 + i, pl.ds(row, 1), :]
            return 0

        return lax.fori_loop(0, I, body, 0)

    lax.fori_loop(0, J, first_rims, 0)
    for way in (0, 1):
        start("slabs", way, [y_copy(0, way)])
    load_cells.wait()

    def tile(step, j, i):
        old, new = grids[step - 1], grids[step]
        middle = old[1 + j, 1 + i]
        before = y_in[step - 1, 0, j, pl.ds(i, 1), :]
        after = y_in[step - 1, 1, j, pl.ds(i, 1), :]
        near = jnp.concatenate([before, middle[: K - 1]], axis=0)
        far = jnp.concatenate([middle[1:], after], axis=0)
        around = (
            (old[j, 1 + i] + old[2 + j, 1 + i])
            + (old[1 + j, i] + old[1 + j, 2 + i])
            + (near + far)
        )
        value = middle * (0.6 - 0.2 * (middle * cells[j, i])) + 0.1 * around
        if step < STEPS:
            new[1 + j, 1 + i] = value
            rims(step, j, i, value)
        else:
            new[j, i] = value

    for step in range(1, STEPS + 1):
        last = step == STEPS
        for way in (0, 1):
            arrived("slabs", way, [y_copy(step - 1, way)])

        def inner(j, _):
            def body(i, _):
                tile(step, j, i)
                return 0

            return lax.fori_loop(1, I - 1, body, 0)

        lax.fori_loop(1, J - 1, inner, 0)
        for way in (0, 1):
            arrived("cols", way, [z_copy(step - 1, way, part) for part in range(3)])

        def edges(j, _):
            tile(step, j, 0)
            tile(step, j, I - 1)
            return 0

        lax.fori_loop(1, J - 1, edges, 0)
        if not last:
            for way in (0, 1):
                start("cols", way, [z_copy(step, way, 1)])
        for q in range(Q):
            for way in (0, 1):
                arrived("rows", way, [x_copy(step - 1, way, q)])

            def faces(i, _):
                tile(step, 0, i)
                tile(step, J - 1, i)
                return 0

            lax.fori_loop(q * W, (q + 1) * W, faces, 0)
            if not last:
                for way in (0, 1):
                    start("rows", way, [x_copy(step, way, q)])
            else:
                columns = pl.ds(q * W, W)

                @pl.when(has_target["rows"][0])
                def _():
                    def add(i, _):
                        value = grid3[0, i]
                        for j in range(1, J):
                            value = value + grid3[j, i]
                        total[i] = value
                        return 0

                    lax.fori_loop(q * W, (q + 1) * W, add, 0)

                @pl.when(jnp.logical_not(has_source["rows"][0]))
                def _():
                    start("rows", 0, [t_copy(q)])

                pltpu.make_async_copy(
                    grid3.at[:, columns], out_field.at[:, columns], store.at[0, q]
                ).start()
        if not last:
            for way in (0, 1):
                start("cols", way, [z_copy(step, way, 0), z_copy(step, way, 2)])
                start("slabs", way, [y_copy(step, way)])

    for q in range(Q):
        columns = pl.ds(q * W, W)

        @pl.when(has_source["rows"][0])
        def _():
            if sizes["rows"] > 1:
                t_copy(q).wait_recv()

                @pl.when(has_target["rows"][0])
                def _():
                    def add(i, _):
                        total[i] = total[i] + below[i]
                        return 0

                    lax.fori_loop(q * W, (q + 1) * W, add, 0)
                    t_copy(q).start()

        pltpu.make_async_copy(
            below.at[columns], out_below.at[columns], store.at[1, q]
        ).start()

    for step in range(STEPS):
        for way in (0, 1):
            sent("rows", way, [x_copy(step, way, q) for q in range(Q)])
            sent("cols", way, [z_copy(step, way, part) for part in range(3)])
            sent("slabs", way, [y_copy(step, way)])
    sent("rows", 0, [t_copy(q) for q in range(Q)])
    for q in range(Q):
        columns = pl.ds(q * W, W)
        pltpu.make_async_copy(
            grid3.at[:, columns], out_field.at[:, columns], store.at[0, q]
        ).wait()
        pltpu.make_async_copy(
            below.at[columns], out_below.at[columns], store.at[1, q]
        ).wait()


def sum_kernel(scale, field, below, potential, field_end):
    J, W = field.shape[0], field.shape[1]

    def body(i, _):
        value = below[i]
        for j in range(J):
            here = field[j, i]
            field_end[j, i] = here
            value = value + here
            potential[j, i] = value * scale
        return 0

    lax.fori_loop(0, W, body, 0)


def solution(mesh):
    sizes = {axis: mesh.shape[axis] for axis in AXES}

    def on_device(field_values, crowding):
        J, I, K, L = field_values.shape
        Q = pieces_of(I)
        padded = pltpu.VMEM((J + 2, I + 2, K, L), jnp.float32)
        block = jax.ShapeDtypeStruct((J, I, K, L), jnp.float32)
        plane = jax.ShapeDtypeStruct((I, K, L), jnp.float32)
        anywhere = pl.BlockSpec(memory_space=pl.ANY)
        dma = pltpu.SemaphoreType.DMA
        field_end, below = pl.pallas_call(
            functools.partial(march_kernel, sizes),
            out_shape=(block, plane),
            in_specs=[anywhere] * 2,
            out_specs=(anywhere, anywhere),
            scratch_shapes=[
                padded,
                padded,
                padded,
                pltpu.VMEM((J, I, K, L), jnp.float32),
                pltpu.VMEM((J, I, K, L), jnp.float32),
                pltpu.VMEM((STEPS, 2, J, I, L), jnp.float32),
                pltpu.VMEM((STEPS, 2, J, I, L), jnp.float32),
                pltpu.VMEM((I, K, L), jnp.float32),
                pltpu.VMEM((I, K, L), jnp.float32),
                dma((STEPS, 2, Q)),
                dma((STEPS, 2, Q)),
                dma((STEPS, 2, 3)),
                dma((STEPS, 2, 3)),
                dma((STEPS, 2)),
                dma((STEPS, 2)),
                dma((Q,)),
                dma((Q,)),
                dma((2,)),
                dma((2, Q)),
            ],
            compiler_params=pltpu.CompilerParams(
                collective_id=0,
                has_side_effects=True,
                vmem_limit_bytes=60 * 1024 * 1024,
            ),
        )(field_values, crowding)

        W = 2 if I % 2 == 0 else 1
        spec = pl.BlockSpec((J, W, K, L), lambda i: (0, i, 0, 0))
        potential, field_end = pl.pallas_call(
            functools.partial(sum_kernel, 1.0 / (J * sizes["rows"])),
            out_shape=(block, block),
            grid=(I // W,),
            in_specs=[spec, pl.BlockSpec((W, K, L), lambda i: (i, 0, 0))],
            out_specs=(spec, spec),
        )(field_end, below)
        return potential, field_end

    spec = P(("trial", "rows"), "cols", "slabs", None)
    return jax.shard_map(
        on_device,
        mesh=mesh,
        in_specs=(spec, spec),
        out_specs=(spec, spec),
        check_vma=False,
    )
```

```python
import functools

import jax
import jax.numpy as jnp
from jax import lax
from jax.experimental import pallas as pl
from jax.experimental.pallas import tpu as pltpu
from jax.sharding import PartitionSpec as P

STEPS = 3
MESH = pl.DeviceIdType.MESH
AXES = ("rows", "cols", "slabs")


def pieces_of(length):
    for count in (4, 2):
        if length % count == 0:
            return count
    return 1


def march_kernel(
    sizes, field, crowd, grid3, out_below,
    grid0, grid1, grid2, cells, y_in, y_out, total, below,
    x_send, x_recv, z_send, z_recv, y_send, y_recv, t_send, t_recv, load,
):
    J, I, K, L = field.shape
    grids = (grid0, grid1, grid2, grid3)
    Q = pieces_of(I)
    W = I // Q
    place = {axis: lax.axis_index(axis) for axis in AXES}
    has_target = {}
    has_source = {}
    for axis in AXES:
        later, earlier = place[axis] < sizes[axis] - 1, place[axis] > 0
        has_target[axis] = (later, earlier)
        has_source[axis] = (earlier, later)

    def target(axis, way):
        n = sizes[axis]
        return {axis: lax.rem(place[axis] + (1 if way == 0 else n - 1), n)}

    load_field = pltpu.make_async_copy(
        field, grid0.at[1 : J + 1, 1 : I + 1], load.at[0]
    )
    load_cells = pltpu.make_async_copy(crowd, cells, load.at[1])
    load_field.start()

    barrier = pltpu.get_barrier_semaphore()
    for axis in AXES:
        if sizes[axis] > 1:
            for way in (0, 1):

                @pl.when(has_target[axis][way])
                def _():
                    pl.semaphore_signal(
                        barrier, inc=1, device_id=target(axis, way), device_id_type=MESH
                    )

    peers = jnp.int32(0)
    for axis in AXES:
        if sizes[axis] > 1:
            for way in (0, 1):
                peers = peers + has_source[axis][way].astype(jnp.int32)
    pl.semaphore_wait(barrier, peers)

    def x_copy(step, way, q):
        plane = J - 1 if way == 0 else 0
        halo = 0 if way == 0 else J + 1
        columns = pl.ds(1 + q * W, W)
        if step == 0:
            source = field.at[plane, pl.ds(q * W, W)]
        else:
            source = grids[step].at[1 + plane, columns]
        return pltpu.make_async_remote_copy(
            src_ref=source,
            dst_ref=grids[step].at[halo, columns],
            send_sem=x_send.at[step, way, q],
            recv_sem=x_recv.at[step, way, q],
            device_id=target("rows", way),
            device_id_type=MESH,
        )

    parts = ((0, 1), (1, J - 2), (J - 1, 1))

    def z_copy(step, way, part):
        first, count = parts[part]
        column = I - 1 if way == 0 else 0
        halo = 0 if way == 0 else I + 1
        if step == 0:
            source = field.at[pl.ds(first, count), column]
        else:
            source = grids[step].at[pl.ds(1 + first, count), 1 + column]
        return pltpu.make_async_remote_copy(
            src_ref=source,
            dst_ref=grids[step].at[pl.ds(1 + first, count), halo],
            send_sem=z_send.at[step, way, part],
            recv_sem=z_recv.at[step, way, part],
            device_id=target("cols", way),
            device_id_type=MESH,
        )

    def y_copy(step, way):
        return pltpu.make_async_remote_copy(
            src_ref=y_out.at[step, 1 - way],
            dst_ref=y_in.at[step, way],
            send_sem=y_send.at[step, way],
            recv_sem=y_recv.at[step, way],
            device_id=target("slabs", way),
            device_id_type=MESH,
        )

    def t_copy(q):
        columns = pl.ds(q * W, W)
        return pltpu.make_async_remote_copy(
            src_ref=total.at[columns],
            dst_ref=below.at[columns],
            send_sem=t_send.at[q],
            recv_sem=t_recv.at[q],
            device_id=target("rows", 0),
            device_id_type=MESH,
        )

    def start(axis, way, copies):
        if sizes[axis] > 1:

            @pl.when(has_target[axis][way])
            def _():
                for one in copies:
                    one.start()

    def sent(axis, way, copies):
        if sizes[axis] > 1:

            @pl.when(has_target[axis][way])
            def _():
                for one in copies:
                    one.wait_send()

    def arrived(axis, way, copies):
        if sizes[axis] > 1:

            @pl.when(has_source[axis][way])
            def _():
                for one in copies:
                    one.wait_recv()

    for way in (0, 1):
        start("cols", way, [z_copy(0, way, part) for part in range(3)])
    for q in range(Q):
        for way in (0, 1):
            start("rows", way, [x_copy(0, way, q)])
    load_cells.start()

    zero = jnp.zeros((K, L), jnp.float32)
    for way in (0, 1):

        @pl.when(jnp.logical_not(has_source["rows"][way]))
        def _():
            def body(i, _):
                for step in range(STEPS):
                    grids[step][0 if way == 0 else J + 1, 1 + i] = zero
                if way == 0:
                    below[i] = zero
                return 0

            lax.fori_loop(0, I, body, 0)

        @pl.when(jnp.logical_not(has_source["cols"][way]))
        def _():
            def body(j, _):
                for step in range(STEPS):
                    grids[step][1 + j, 0 if way == 0 else I + 1] = zero
                return 0

            lax.fori_loop(0, J, body, 0)

        @pl.when(jnp.logical_not(has_source["slabs"][way]))
        def _():
            for step in range(STEPS):
                y_in[step, way] = jnp.zeros((J, I, L), jnp.float32)

    load_field.wait()

    def rims(step, j, i, value):
        y_out[step, 0, j, pl.ds(i, 1), :] = value[0:1]
        y_out[step, 1, j, pl.ds(i, 1), :] = value[K - 1 : K]

    def first_rims(j, _):
        def body(i, _):
            for side, row in ((0, 0), (1, K - 1)):
                y_out[0, side, j, pl.ds(i, 1), :] = grid0[1 + j, 1 + i, pl.ds(row, 1), :]
            return 0

        return lax.fori_loop(0, I, body, 0)

    lax.fori_loop(0, J, first_rims, 0)
    for way in (0, 1):
        start("slabs", way, [y_copy(0, way)])
    load_cells.wait()

    def tile(step, j, i):
        old, new = grids[step - 1], grids[step]
        middle = old[1 + j, 1 + i]
        before = y_in[step - 1, 0, j, pl.ds(i, 1), :]
        after = y_in[step - 1, 1, j, pl.ds(i, 1), :]
        near = jnp.concatenate([before, middle[: K - 1]], axis=0)
        far = jnp.concatenate([middle[1:], after], axis=0)
        around = (
            (old[j, 1 + i] + old[2 + j, 1 + i])
            + (old[1 + j, i] + old[1 + j, 2 + i])
            + (near + far)
        )
        value = middle * (0.6 - 0.2 * (middle * cells[j, i])) + 0.1 * around
        if step < STEPS:
            new[1 + j, 1 + i] = value
            rims(step, j, i, value)
        else:
            new[j, i] = value

    for step in range(1, STEPS + 1):
        last = step == STEPS
        for way in (0, 1):
            arrived("slabs", way, [y_copy(step - 1, way)])

        def inner(j, _):
            def body(i, _):
                tile(step, j, i)
                return 0

            return lax.fori_loop(1, I - 1, body, 0)

        lax.fori_loop(1, J - 1, inner, 0)
        for way in (0, 1):
            arrived("cols", way, [z_copy(step - 1, way, part) for part in range(3)])

        def edges(j, _):
            tile(step, j, 0)
            tile(step, j, I - 1)
            return 0

        lax.fori_loop(1, J - 1, edges, 0)
        if not last:
            for way in (0, 1):
                start("cols", way, [z_copy(step, way, 1)])
        for q in range(Q):
            for way in (0, 1):
                arrived("rows", way, [x_copy(step - 1, way, q)])

            def faces(i, _):
                tile(step, 0, i)
                tile(step, J - 1, i)
                return 0

            lax.fori_loop(q * W, (q + 1) * W, faces, 0)
            if not last:
                for way in (0, 1):
                    start("rows", way, [x_copy(step, way, q)])
            else:

                @pl.when(has_target["rows"][0])
                def _():
                    def add(i, _):
                        value = grid3[0, i]
                        for j in range(1, J):
                            value = value + grid3[j, i]
                        total[i] = value
                        return 0

                    lax.fori_loop(q * W, (q + 1) * W, add, 0)

                @pl.when(jnp.logical_not(has_source["rows"][0]))
                def _():
                    start("rows", 0, [t_copy(q)])
        if not last:
            for way in (0, 1):
                start("cols", way, [z_copy(step, way, 0), z_copy(step, way, 2)])
                start("slabs", way, [y_copy(step, way)])

    for q in range(Q):

        @pl.when(has_source["rows"][0])
        def _():
            if sizes["rows"] > 1:
                t_copy(q).wait_recv()

                @pl.when(has_target["rows"][0])
                def _():
                    def add(i, _):
                        total[i] = total[i] + below[i]
                        return 0

                    lax.fori_loop(q * W, (q + 1) * W, add, 0)
                    t_copy(q).start()

        columns = pl.ds(q * W, W)
        out_below[columns] = below[columns]

    for step in range(STEPS):
        for way in (0, 1):
            sent("rows", way, [x_copy(step, way, q) for q in range(Q)])
            sent("cols", way, [z_copy(step, way, part) for part in range(3)])
            sent("slabs", way, [y_copy(step, way)])
    sent("rows", 0, [t_copy(q) for q in range(Q)])

def sum_kernel(scale, field, below, potential, field_end, sums, end_sem, sum_sem):
    J, I = field.shape[0], field.shape[1]
    Q = pieces_of(I)
    W = I // Q
    whole = pltpu.make_async_copy(field, field_end, end_sem)
    whole.start()

    def piece(q):
        columns = pl.ds(q * W, W)
        return pltpu.make_async_copy(
            sums.at[:, columns], potential.at[:, columns], sum_sem.at[q]
        )

    for q in range(Q):

        def body(i, _):
            value = below[i]
            for j in range(J):
                value = value + field[j, i]
                sums[j, i] = value * scale
            return 0

        lax.fori_loop(q * W, (q + 1) * W, body, 0)
        piece(q).start()
    for q in range(Q):
        piece(q).wait()
    whole.wait()


def solution(mesh):
    sizes = {axis: mesh.shape[axis] for axis in AXES}

    def on_device(field_values, crowding):
        J, I, K, L = field_values.shape
        Q = pieces_of(I)
        padded = pltpu.VMEM((J + 2, I + 2, K, L), jnp.float32)
        block = jax.ShapeDtypeStruct((J, I, K, L), jnp.float32)
        vector = pl.BlockSpec(memory_space=pltpu.VMEM)
        anywhere = pl.BlockSpec(memory_space=pl.ANY)
        dma = pltpu.SemaphoreType.DMA
        field_end, below = pl.pallas_call(
            functools.partial(march_kernel, sizes),
            out_shape=(
                pltpu.VMEM((J, I, K, L), jnp.float32),
                pltpu.VMEM((I, K, L), jnp.float32),
            ),
            in_specs=[anywhere] * 2,
            out_specs=(vector, vector),
            scratch_shapes=[
                padded,
                padded,
                padded,
                pltpu.VMEM((J, I, K, L), jnp.float32),
                pltpu.VMEM((STEPS, 2, J, I, L), jnp.float32),
                pltpu.VMEM((STEPS, 2, J, I, L), jnp.float32),
                pltpu.VMEM((I, K, L), jnp.float32),
                pltpu.VMEM((I, K, L), jnp.float32),
                dma((STEPS, 2, Q)),
                dma((STEPS, 2, Q)),
                dma((STEPS, 2, 3)),
                dma((STEPS, 2, 3)),
                dma((STEPS, 2)),
                dma((STEPS, 2)),
                dma((Q,)),
                dma((Q,)),
                dma((2,)),
            ],
            compiler_params=pltpu.CompilerParams(
                collective_id=0,
                has_side_effects=True,
                vmem_limit_bytes=57 * 1024 * 1024,
            ),
        )(field_values, crowding)

        potential, field_end = pl.pallas_call(
            functools.partial(sum_kernel, 1.0 / (J * sizes["rows"])),
            out_shape=(block, block),
            in_specs=[vector, vector],
            out_specs=(anywhere, anywhere),
            scratch_shapes=[pltpu.VMEM((J, I, K, L), jnp.float32), dma, dma((Q,))],
            compiler_params=pltpu.CompilerParams(vmem_limit_bytes=16 * 1024 * 1024),
        )(field_end, below)
        return potential, field_end

    spec = P(("trial", "rows"), "cols", "slabs", None)
    return jax.shard_map(
        on_device,
        mesh=mesh,
        in_specs=(spec, spec),
        out_specs=(spec, spec),
        check_vma=False,
    )
```

```python
import functools

import jax
import jax.numpy as jnp
from jax import lax
from jax.experimental import pallas as pl
from jax.experimental.pallas import tpu as pltpu
from jax.sharding import PartitionSpec as P

STEPS = 3
MESH = pl.DeviceIdType.MESH
AXES = ("rows", "cols", "slabs")


def pieces_of(length, counts):
    for count in counts:
        if length % count == 0:
            return count
    return 1


def march_kernel(
    sizes, field, crowd, grid3, out_below,
    grid0, grid1, grid2, cells, y_in, y_out, total, below,
    x_send, x_recv, z_send, z_recv, y_send, y_recv, t_send, t_recv, load, face,
):
    J, I, K, L = field.shape
    grids = (grid0, grid1, grid2, grid3)
    Q = pieces_of(I, (2,))
    W = I // Q
    place = {axis: lax.axis_index(axis) for axis in AXES}
    has_target = {}
    has_source = {}
    for axis in AXES:
        later, earlier = place[axis] < sizes[axis] - 1, place[axis] > 0
        has_target[axis] = (later, earlier)
        has_source[axis] = (earlier, later)

    def target(axis, way):
        n = sizes[axis]
        return {axis: lax.rem(place[axis] + (1 if way == 0 else n - 1), n)}

    def face_load(way, q):
        plane = J - 1 if way == 0 else 0
        return pltpu.make_async_copy(
            field.at[plane, pl.ds(q * W, W)],
            grid0.at[1 + plane, pl.ds(1 + q * W, W)],
            face.at[way, q],
        )

    load_field = pltpu.make_async_copy(
        field.at[1 : J - 1], grid0.at[2:J, 1 : I + 1], load.at[0]
    )
    load_cells = pltpu.make_async_copy(crowd, cells, load.at[1])
    for q in range(Q):
        for way in (0, 1):
            face_load(way, q).start()

    barrier = pltpu.get_barrier_semaphore()
    for axis in AXES:
        if sizes[axis] > 1:
            for way in (0, 1):

                @pl.when(has_target[axis][way])
                def _():
                    pl.semaphore_signal(
                        barrier, inc=1, device_id=target(axis, way), device_id_type=MESH
                    )

    peers = jnp.int32(0)
    for axis in AXES:
        if sizes[axis] > 1:
            for way in (0, 1):
                peers = peers + has_source[axis][way].astype(jnp.int32)
    pl.semaphore_wait(barrier, peers)

    def x_copy(step, way, q):
        plane = J - 1 if way == 0 else 0
        halo = 0 if way == 0 else J + 1
        columns = pl.ds(1 + q * W, W)
        return pltpu.make_async_remote_copy(
            src_ref=grids[step].at[1 + plane, columns],
            dst_ref=grids[step].at[halo, columns],
            send_sem=x_send.at[step, way, q],
            recv_sem=x_recv.at[step, way, q],
            device_id=target("rows", way),
            device_id_type=MESH,
        )

    parts = ((0, 1), (1, J - 2), (J - 1, 1))

    def z_copy(step, way, part):
        first, count = parts[part]
        column = I - 1 if way == 0 else 0
        halo = 0 if way == 0 else I + 1
        if step == 0:
            source = field.at[pl.ds(first, count), column]
        else:
            source = grids[step].at[pl.ds(1 + first, count), 1 + column]
        return pltpu.make_async_remote_copy(
            src_ref=source,
            dst_ref=grids[step].at[pl.ds(1 + first, count), halo],
            send_sem=z_send.at[step, way, part],
            recv_sem=z_recv.at[step, way, part],
            device_id=target("cols", way),
            device_id_type=MESH,
        )

    def y_copy(step, way):
        return pltpu.make_async_remote_copy(
            src_ref=y_out.at[step, 1 - way],
            dst_ref=y_in.at[step, way],
            send_sem=y_send.at[step, way],
            recv_sem=y_recv.at[step, way],
            device_id=target("slabs", way),
            device_id_type=MESH,
        )

    def t_copy(q):
        columns = pl.ds(q * W, W)
        return pltpu.make_async_remote_copy(
            src_ref=total.at[columns],
            dst_ref=below.at[columns],
            send_sem=t_send.at[q],
            recv_sem=t_recv.at[q],
            device_id=target("rows", 0),
            device_id_type=MESH,
        )

    def start(axis, way, copies):
        if sizes[axis] > 1:

            @pl.when(has_target[axis][way])
            def _():
                for one in copies:
                    one.start()

    def sent(axis, way, copies):
        if sizes[axis] > 1:

            @pl.when(has_target[axis][way])
            def _():
                for one in copies:
                    one.wait_send()

    def arrived(axis, way, copies):
        if sizes[axis] > 1:

            @pl.when(has_source[axis][way])
            def _():
                for one in copies:
                    one.wait_recv()

    for q in range(Q):
        for way in (0, 1):
            face_load(way, q).wait()
            start("rows", way, [x_copy(0, way, q)])
    for way in (0, 1):
        start("cols", way, [z_copy(0, way, part) for part in range(3)])
    load_field.start()
    load_cells.start()

    zero = jnp.zeros((K, L), jnp.float32)
    for way in (0, 1):

        @pl.when(jnp.logical_not(has_source["rows"][way]))
        def _():
            def body(i, _):
                for step in range(STEPS):
                    grids[step][0 if way == 0 else J + 1, 1 + i] = zero
                if way == 0:
                    below[i] = zero
                return 0

            lax.fori_loop(0, I, body, 0)

        @pl.when(jnp.logical_not(has_source["cols"][way]))
        def _():
            def body(j, _):
                for step in range(STEPS):
                    grids[step][1 + j, 0 if way == 0 else I + 1] = zero
                return 0

            lax.fori_loop(0, J, body, 0)

        @pl.when(jnp.logical_not(has_source["slabs"][way]))
        def _():
            for step in range(STEPS):
                y_in[step, way] = jnp.zeros((J, I, L), jnp.float32)

    load_field.wait()

    def rims(step, j, i, value):
        y_out[step, 0, j, pl.ds(i, 1), :] = value[0:1]
        y_out[step, 1, j, pl.ds(i, 1), :] = value[K - 1 : K]

    def first_rims(j, _):
        def body(i, _):
            for side, row in ((0, 0), (1, K - 1)):
                y_out[0, side, j, pl.ds(i, 1), :] = grid0[1 + j, 1 + i, pl.ds(row, 1), :]
            return 0

        return lax.fori_loop(0, I, body, 0)

    lax.fori_loop(0, J, first_rims, 0)
    for way in (0, 1):
        start("slabs", way, [y_copy(0, way)])
    load_cells.wait()

    def tile(step, j, i):
        old, new = grids[step - 1], grids[step]
        middle = old[1 + j, 1 + i]
        before = y_in[step - 1, 0, j, pl.ds(i, 1), :]
        after = y_in[step - 1, 1, j, pl.ds(i, 1), :]
        near = jnp.concatenate([before, middle[: K - 1]], axis=0)
        far = jnp.concatenate([middle[1:], after], axis=0)
        around = (
            (old[j, 1 + i] + old[2 + j, 1 + i])
            + (old[1 + j, i] + old[1 + j, 2 + i])
            + (near + far)
        )
        value = middle * (0.6 - 0.2 * (middle * cells[j, i])) + 0.1 * around
        if step < STEPS:
            new[1 + j, 1 + i] = value
            rims(step, j, i, value)
        else:
            new[j, i] = value

    for step in range(1, STEPS + 1):
        last = step == STEPS
        for way in (0, 1):
            arrived("slabs", way, [y_copy(step - 1, way)])

        def inner(j, _):
            def body(i, _):
                tile(step, j, i)
                return 0

            return lax.fori_loop(1, I - 1, body, 0)

        lax.fori_loop(1, J - 1, inner, 0)
        for way in (0, 1):
            arrived("cols", way, [z_copy(step - 1, way, part) for part in range(3)])

        def edges(j, _):
            tile(step, j, 0)
            tile(step, j, I - 1)
            return 0

        lax.fori_loop(1, J - 1, edges, 0)
        if not last:
            for way in (0, 1):
                start("cols", way, [z_copy(step, way, 1)])
        for q in range(Q):
            for way in (0, 1):
                arrived("rows", way, [x_copy(step - 1, way, q)])

            def faces(i, _):
                tile(step, 0, i)
                tile(step, J - 1, i)
                return 0

            lax.fori_loop(q * W, (q + 1) * W, faces, 0)
            if not last:
                for way in (0, 1):
                    start("rows", way, [x_copy(step, way, q)])
            else:

                @pl.when(has_target["rows"][0])
                def _():
                    def add(i, _):
                        value = grid3[0, i]
                        for j in range(1, J):
                            value = value + grid3[j, i]
                        total[i] = value
                        return 0

                    lax.fori_loop(q * W, (q + 1) * W, add, 0)

                @pl.when(jnp.logical_not(has_source["rows"][0]))
                def _():
                    start("rows", 0, [t_copy(q)])
        if not last:
            for way in (0, 1):
                start("cols", way, [z_copy(step, way, 0), z_copy(step, way, 2)])
                start("slabs", way, [y_copy(step, way)])

    for q in range(Q):

        @pl.when(has_source["rows"][0])
        def _():
            if sizes["rows"] > 1:
                t_copy(q).wait_recv()

                @pl.when(has_target["rows"][0])
                def _():
                    def add(i, _):
                        total[i] = total[i] + below[i]
                        return 0

                    lax.fori_loop(q * W, (q + 1) * W, add, 0)
                    t_copy(q).start()

        columns = pl.ds(q * W, W)
        out_below[columns] = below[columns]

    for step in range(STEPS):
        for way in (0, 1):
            sent("rows", way, [x_copy(step, way, q) for q in range(Q)])
            sent("cols", way, [z_copy(step, way, part) for part in range(3)])
            sent("slabs", way, [y_copy(step, way)])
    sent("rows", 0, [t_copy(q) for q in range(Q)])

def sum_kernel(scale, field, below, potential, field_end, sums, end_sem, sum_sem):
    J, I = field.shape[0], field.shape[1]
    Q = pieces_of(I, (4, 2))
    W = I // Q

    whole = pltpu.make_async_copy(field, field_end, end_sem)
    whole.start()

    def piece(q):
        columns = pl.ds(q * W, W)
        return pltpu.make_async_copy(
            sums.at[:, columns], potential.at[:, columns], sum_sem.at[q]
        )

    for q in range(Q):

        def body(i, _):
            value = below[i]
            for j in range(J):
                value = value + field[j, i]
                sums[j, i] = value * scale
            return 0

        lax.fori_loop(q * W, (q + 1) * W, body, 0)
        piece(q).start()
    for q in range(Q):
        piece(q).wait()
    whole.wait()


def solution(mesh):
    sizes = {axis: mesh.shape[axis] for axis in AXES}

    def on_device(field_values, crowding):
        J, I, K, L = field_values.shape
        Q = pieces_of(I, (2,))
        padded = pltpu.VMEM((J + 2, I + 2, K, L), jnp.float32)
        block = jax.ShapeDtypeStruct((J, I, K, L), jnp.float32)
        vector = pl.BlockSpec(memory_space=pltpu.VMEM)
        anywhere = pl.BlockSpec(memory_space=pl.ANY)
        dma = pltpu.SemaphoreType.DMA
        field_end, below = pl.pallas_call(
            functools.partial(march_kernel, sizes),
            out_shape=(
                pltpu.VMEM((J, I, K, L), jnp.float32),
                pltpu.VMEM((I, K, L), jnp.float32),
            ),
            in_specs=[anywhere] * 2,
            out_specs=(vector, vector),
            scratch_shapes=[
                padded,
                padded,
                padded,
                pltpu.VMEM((J, I, K, L), jnp.float32),
                pltpu.VMEM((STEPS, 2, J, I, L), jnp.float32),
                pltpu.VMEM((STEPS, 2, J, I, L), jnp.float32),
                pltpu.VMEM((I, K, L), jnp.float32),
                pltpu.VMEM((I, K, L), jnp.float32),
                dma((STEPS, 2, Q)),
                dma((STEPS, 2, Q)),
                dma((STEPS, 2, 3)),
                dma((STEPS, 2, 3)),
                dma((STEPS, 2)),
                dma((STEPS, 2)),
                dma((Q,)),
                dma((Q,)),
                dma((2,)),
                dma((2, Q)),
            ],
            compiler_params=pltpu.CompilerParams(
                collective_id=0,
                has_side_effects=True,
                vmem_limit_bytes=57 * 1024 * 1024,
            ),
        )(field_values, crowding)

        potential, field_end = pl.pallas_call(
            functools.partial(sum_kernel, 1.0 / (J * sizes["rows"])),
            out_shape=(block, block),
            in_specs=[vector, vector],
            out_specs=(anywhere, anywhere),
            scratch_shapes=[pltpu.VMEM((J, I, K, L), jnp.float32), dma, dma((pieces_of(I, (4, 2)),))],
            compiler_params=pltpu.CompilerParams(vmem_limit_bytes=16 * 1024 * 1024),
        )(field_end, below)
        return potential, field_end

    spec = P(("trial", "rows"), "cols", "slabs", None)
    return jax.shard_map(
        on_device,
        mesh=mesh,
        in_specs=(spec, spec),
        out_specs=(spec, spec),
        check_vma=False,
    )
```
